32 devices in a mesh: basin: 4 (over z), reach: 8 (over y, x, core).
Axes of the slice: x: 2, y: 2, z: 4, core: 2. Of those that a mesh axis runs over, the one named last changes fastest.
Arguments:
- sensitivity: float32 [16, 128, 256], P(None, ('basin', 'reach')), may hold values from -6 to 6
- inverse: float32 [128, 256, 256], P(('basin', 'reach')), may hold values from -0.375 to 0.375
- spread: float32 [128, 256], P(('basin', 'reach')), may hold values from -3 to 3
- gather_weight: float32 [128, 256], P(('basin', 'reach')), may hold values from -0.0625 to 0.0625
- retain: float32 [128], P(('basin', 'reach')), may hold values from 0.984375 to 1
- storage: float32 [128, 256], P(('basin', 'reach')), may hold values from 0.2 to 0.6
- conf_source: int32 [32, 8, 64], P(('basin', 'reach')), may hold values from 0 to 1023
- conf_target: int32 [32, 8, 64], P(('basin', 'reach')), may hold values from 0 to 1023
- conf_weight: float32 [32, 8, 64], P(('basin', 'reach')), may hold values from 0.1 to 0.4
Outputs:
- adjoint: float32 [16, 128, 256], P(None, ('basin', 'reach'))
The draws below stay inside these ranges and needn't reach their ends.
All inputs are finite; a program needn't handle non-finite values.
Results may differ from the reference program's by a relative error of at most 0.00019.
Values sent between devices are 32-bit elements; how exact they have to be, the bound alone decides.
No kernel may reach another device: no remote copies, remote signals or barrier semaphores. Data moves between devices by JAX's collectives and lax.ppermute only.
A program may use at most 64 MiB of HBM per device.

```python
import jax
import jax.numpy as jnp
from jax import lax

R = 256
NB = 4
F = 64
STEPS = 16
PEERS = 8
DEV_COUNT = 32
BLOCKS = 128


def touch_ends(drawn, own_key, least, top_value):
    spot = [jax.random.randint(jax.random.fold_in(own_key, axis), (), 0, length) for axis, length in enumerate(drawn.shape)]
    longest = drawn.shape.index(max(drawn.shape))
    next_to = spot[:longest] + [(spot[longest] + 1) % drawn.shape[longest]] + spot[longest + 1:]
    return drawn.at[tuple(spot)].set(least).at[tuple(next_to)].set(top_value)


def block_scale(stream_key, shape, split, smallest, top_value):
    factor_of = 1.0
    for position, parts in split:
        draws = jax.random.uniform(jax.random.fold_in(jax.random.fold_in(stream_key, 6), position), (parts,), jnp.float32, smallest / len(split), top_value / len(split))
        factor_of = factor_of * jnp.repeat(jnp.exp(draws), shape[position] // parts).reshape((-1,) + (1,) * (len(shape) - 1 - position))
    return factor_of


def centred(stream_key, extent, scale, most, split=(), held_as=jnp.bfloat16):
    drawn = jax.random.normal(stream_key, extent, jnp.float32) * scale
    if len(split) > 0:
        drawn = block_scale(stream_key, extent, split, -0.22, 0.18) * drawn
    return jnp.clip(drawn, min=-most, max=most).astype(held_as)


def setup_inputs(seed: int = 0) -> dict:
    keys = jax.random.split(jax.random.key(seed), 10)
    sensitivity = centred(keys[0], (STEPS, BLOCKS, R), 1.0, 6.0, ((1, 32),), jnp.float32)
    inverse = centred(keys[1], (BLOCKS, R, R), R ** -0.5, 0.375, ((0, 32),), jnp.float32)
    spread = centred(keys[2], (BLOCKS, R), 0.5, 3.0, ((0, 32),), jnp.float32)
    gather_weight = centred(keys[3], (BLOCKS, R), (R * BLOCKS // 4) ** -0.5, 0.0625, ((0, 32),), jnp.float32)
    retain = jnp.clip(0.984375 + 0.015625 * jax.random.uniform(keys[4], (BLOCKS,), jnp.float32) ** block_scale(keys[4], (BLOCKS,), ((0, 32),), -0.2, 0.2), 0.984375, 1.0)
    storage = jnp.clip(0.2 + 0.400000021 * jax.random.uniform(keys[5], (BLOCKS, R), jnp.float32) ** block_scale(keys[5], (BLOCKS, R), ((0, 32),), -0.2, 0.2), 0.2, 0.6)
    conf_source = touch_ends(jax.random.randint(keys[6], (DEV_COUNT, PEERS, F), 0, NB * R), jax.random.fold_in(keys[6], 1), 0, (NB * R) - 1).astype(jnp.int32)
    conf_target = touch_ends(jax.random.randint(keys[7], (DEV_COUNT, PEERS, F), 0, NB * R), jax.random.fold_in(keys[7], 1), 0, (NB * R) - 1).astype(jnp.int32)
    conf_weight = jnp.clip(0.1 + 0.3 * jax.random.uniform(keys[8], (DEV_COUNT, PEERS, F), jnp.float32) ** block_scale(keys[8], (DEV_COUNT, PEERS, F), ((0, 32),), -0.2, 0.2), 0.1, 0.4)
    return {"sensitivity": sensitivity, "inverse": inverse, "spread": spread, "gather_weight": gather_weight, "retain": retain, "storage": storage, "conf_source": conf_source, "conf_target": conf_target, "conf_weight": conf_weight}


def reference(sensitivity, inverse, spread, gather_weight, retain, storage, conf_source, conf_target, conf_weight):
    rows = NB * R
    group = (jnp.arange(DEV_COUNT, dtype=jnp.int32) // PEERS) * PEERS
    src_dev = jnp.broadcast_to(group[:, None, None] + jnp.arange(PEERS, dtype=jnp.int32)[None, :, None], conf_source.shape)
    dev_ids = jnp.broadcast_to(jnp.arange(DEV_COUNT, dtype=jnp.int32)[:, None, None], conf_target.shape)

    def step(later, forcing_now):
        flat = later.reshape(DEV_COUNT, rows)
        values = flat[src_dev, conf_source] * conf_weight
        fan = jnp.zeros((DEV_COUNT, rows), jnp.float32).at[dev_ids, conf_target].add(values)
        forcing = forcing_now + storage * later + fan.reshape(BLOCKS, R)
        local = jnp.einsum("bij,bi->bj", inverse, forcing, precision=lax.Precision.HIGHEST)
        feed = jnp.sum(gather_weight * local, axis=1)

        def link(stem, pair):
            keep, term = pair
            return keep * stem + term, stem

        _, stem_next = lax.scan(link, jnp.zeros((), jnp.float32), (retain, feed), reverse=True)
        adjoint = local + spread * stem_next[:, None]
        return adjoint, adjoint

    _, adjoint = lax.scan(step, jnp.zeros((BLOCKS, R), jnp.float32), sensitivity, reverse=True)
    return adjoint
```

```python
import functools

import jax
import jax.numpy as jnp
from jax import lax
from jax.experimental import pallas as pl
from jax.experimental.pallas import tpu as pltpu
from jax.sharding import PartitionSpec as P

LANES = 128
SUB = 8
HIGHEST = lax.Precision.HIGHEST
VMEM = pltpu.MemorySpace.VMEM
SMEM = pltpu.MemorySpace.SMEM


def vmem():
    return pl.BlockSpec(memory_space=VMEM)


def smem():
    return pl.BlockSpec(memory_space=SMEM)


def swap(value, axis, bit):
    return lax.ppermute(value, axis, [(i, i ^ bit) for i in range(lax.axis_size(axis))])


def prepare_kernel(inv_ref, gather_ref, sent_ref, upon_ref):
    blocks, reaches, _ = inv_ref.shape
    halves = reaches // LANES
    rows = halves * halves * blocks
    for n in range(blocks):
        for ih in range(halves):
            for h in range(halves):
                row = (ih * halves + h) * blocks + n

                def tile(i, carry, n=n, ih=ih, h=h, row=row):
                    block = inv_ref[n, pl.ds(ih * LANES + i * SUB, SUB), h * LANES : (h + 1) * LANES]
                    sent_ref[pl.ds(i * SUB * rows + row, SUB, stride=rows), :] = block
                    return carry

                lax.fori_loop(0, LANES // SUB, tile, 0, unroll=4)
    for n in range(blocks):
        part = lax.dot_general(
            gather_ref[...], inv_ref[n], (((1,), (1,)), ((), ())),
            precision=HIGHEST, preferred_element_type=jnp.float32,
        )
        for ih in range(halves):
            row = ih * blocks + n
            upon_ref[row : row + 1, :] = part[n : n + 1, ih * LANES : (ih + 1) * LANES]


def prepare(inverse, gather_weight):
    blocks, reaches, _ = inverse.shape
    rows = (reaches // LANES) ** 2 * blocks
    return pl.pallas_call(
        prepare_kernel,
        out_shape=(
            jax.ShapeDtypeStruct((LANES * rows, LANES), jnp.float32),
            jax.ShapeDtypeStruct((SUB, LANES), jnp.float32),
        ),
        in_specs=[vmem(), vmem()],
        out_specs=(vmem(), vmem()),
        name="prepare",
    )(inverse, gather_weight)


def tables_kernel(slots, code_sm, code_ref, next_ref, head_ref, most_ref):
    pairs = code_ref.shape[0]
    levels = next_ref.shape[0]
    lane = lax.broadcasted_iota(jnp.int32, (SUB, LANES), 1)
    within = lax.rem(lane, slots)
    most = jnp.zeros((SUB, LANES), jnp.int32)
    for v in range(pairs):
        code = code_ref[v]
        seen = jnp.zeros((SUB, LANES), jnp.int32)
        nexts = [jnp.full((SUB, LANES), -1, jnp.int32) for _ in range(levels)]
        for d in range(1, slots):
            same = (pltpu.roll(code, LANES - d, 1) == code) & (within + d < slots)
            seen = seen + jnp.where(same, 1, 0)
            for j in range(levels):
                if d >= 1 << j:
                    nexts[j] = jnp.where(same & (seen == 1 << j), lane + d, nexts[j])
        for j in range(levels):
            next_ref[j, v] = nexts[j]
        most = jnp.maximum(most, seen)
    most_ref[...] = most

    place = lax.broadcasted_iota(jnp.int32, (SUB, LANES), 0) * LANES + lane
    owners, sources = head_ref.shape[0], head_ref.shape[1]

    def one(i, carry):
        first = lax.rem(i // sources, LANES // slots) * slots
        table = jnp.full((SUB, LANES), -1, jnp.int32)
        for f in reversed(range(slots)):
            table = jnp.where(place == code_sm[i * slots + f], first + f, table)
        head_ref[i // sources, lax.rem(i, sources)] = table
        return carry

    lax.fori_loop(0, owners * sources, one, 0)


def tables(codes, code_vec, slots):
    owners, sources, _ = codes.shape
    levels = (slots - 1).bit_length()
    return pl.pallas_call(
        functools.partial(tables_kernel, slots),
        out_shape=(
            jax.ShapeDtypeStruct((levels,) + code_vec.shape, jnp.int32),
            jax.ShapeDtypeStruct((owners, sources, SUB, LANES), jnp.int32),
            jax.ShapeDtypeStruct((SUB, LANES), jnp.int32),
        ),
        in_specs=[smem(), vmem()],
        out_specs=(vmem(), vmem(), vmem()),
        name="tables",
    )(codes.reshape(-1), code_vec)


def pick(values, lanes):
    return jnp.take_along_axis(values, lanes, axis=1, mode="promise_in_bounds")


def sweep_kernel(count, steps, at, *refs):
    pieces = refs[1 : 1 + count]
    scal = refs[0]
    aux, slane, srow, weight, nexts, heads, most, links, inflow, mine, theirs, inv, adj, slot, fcol = refs[1 + count :]
    pairs = slane.shape[0]
    levels = nexts.shape[0]
    keep, impulse = scal[0], scal[1]
    half = SUB // 2

    def relay(m, carry):
        z = jnp.concatenate([p[m] for p in pieces], axis=0)
        inv[pl.ds(pl.multiple_of(m * LANES, LANES), LANES), :] = z.T
        return carry

    lax.fori_loop(0, LANES, relay, 0, unroll=4)
    adj[...] = jnp.zeros_like(adj)
    seen = jnp.max(most[...])
    jumps = sum((seen >= (1 << j)).astype(jnp.int32) for j in range(levels))
    lane = lax.broadcasted_iota(jnp.int32, (SUB, LANES), 1)
    upper = lax.broadcasted_iota(jnp.int32, (SUB, LANES), 0) < half

    def step(it, leaving):
        t = steps - 1 - it
        rows = [adj[pl.ds(r, count, stride=SUB), :] for r in range(SUB)]
        vals = []
        for v in range(pairs):
            got = jnp.zeros((SUB, LANES), jnp.float32)
            for r in range(SUB):
                got = jnp.where(srow[v] == r, pick(rows[r], slane[v]), got)
            vals.append(got * weight[v])

        def jump(j, vals):
            out = []
            for v in range(pairs):
                n = nexts[j, v]
                out.append(vals[v] + jnp.where(n >= 0, pick(vals[v], n & (LANES - 1)), 0.0))
            return tuple(out)

        vals = lax.fori_loop(0, jumps, jump, tuple(vals))
        for v in range(pairs):
            slot[v * SUB : (v + 1) * SUB, :] = vals[v]
        force = []
        for k in range(count):
            fan = jnp.zeros((SUB, LANES), jnp.float32)
            for s in range(count):
                row = (k * pairs // count) * SUB + s
                table = heads[k, s]
                got = pick(jnp.broadcast_to(slot[row : row + 1, :], (SUB, LANES)), table & (LANES - 1))
                fan = fan + jnp.where(table >= 0, got, 0.0)
            now = aux[k, pl.ds(pl.multiple_of(t * SUB, SUB), SUB), :] * keep
            own = adj[k * SUB : (k + 1) * SUB, :]
            force.append(now + aux[k, at["storage"] : at["storage"] + SUB, :] * own + fan)
        feed = jnp.concatenate(
            [aux[k, at["upon"] : at["upon"] + SUB, :] * force[k] for k in range(count)], axis=0
        )
        spread_rows = []
        for k in range(count):
            other = pltpu.roll(force[k], half, 0)
            spread_rows.append(jnp.where(upper, force[k], other))
            spread_rows.append(jnp.where(upper, other, force[k]))
        fcol[...] = jnp.concatenate(spread_rows, axis=0).T
        stem = jnp.dot(links[...], feed, precision=HIGHEST, preferred_element_type=jnp.float32)
        stem = jnp.sum(stem, axis=1, keepdims=True)
        stem = stem + inflow[...] * jnp.where(it == 0, impulse, 0.0)

        acc = jnp.zeros((LANES, LANES), jnp.float32)
        for m in range(LANES):
            acc = acc + inv[m * LANES : (m + 1) * LANES, :] * fcol[m : m + 1, :]
        rowed = acc.T
        for k in range(count):
            base = 2 * k * SUB
            local = rowed[base : base + SUB] + rowed[base + SUB : base + 2 * SUB]
            new = local + aux[k, at["spread"] : at["spread"] + SUB, :] * stem[k * SUB : (k + 1) * SUB]
            adj[k * SUB : (k + 1) * SUB, :] = new
            if k == 0:
                mine[t] = new
            if k == 1:
                theirs[t] = new
        return jnp.where(lane == t, stem[count * SUB : (count + 1) * SUB], leaving)

    leaving = lax.fori_loop(0, steps, step, jnp.zeros((SUB, LANES), jnp.float32))
    mine[steps] = leaving
    theirs[steps] = leaving


def sweep(at, steps, scal, pieces, aux, slane, srow, weight, nexts, heads, most, links, inflow):
    count = len(pieces)
    out = jax.ShapeDtypeStruct((steps + 1, SUB, LANES), jnp.float32)
    return pl.pallas_call(
        functools.partial(sweep_kernel, count, steps, at),
        out_shape=(out, out),
        in_specs=[smem()] + [vmem()] * (count + 9),
        out_specs=(vmem(), vmem()),
        scratch_shapes=[
            pltpu.VMEM((LANES * LANES, LANES), jnp.float32),
            pltpu.VMEM((count * SUB, LANES), jnp.float32),
            pltpu.VMEM((slane.shape[0] * SUB, LANES), jnp.float32),
            pltpu.VMEM((LANES, LANES), jnp.float32),
        ],
        compiler_params=pltpu.CompilerParams(vmem_limit_bytes=48 * 1024 * 1024),
        name="sweep",
    )(scal, *pieces, aux, slane, srow, weight, nexts, heads, most, links, inflow)


def join_kernel(steps, blocks, scal, mine, theirs, *refs):
    far, out = refs[:-1], refs[-1]
    plain = scal[0] > 0.0
    entering = jnp.zeros((SUB, LANES), jnp.float32)
    for ref in far:
        ahead = ref[0]
        for d in range(steps):
            shifted = entering if d == 0 else pltpu.roll(entering, LANES - d, 1)
            gain = jnp.broadcast_to(ref[1][:, steps - 1 - d : steps - d], (SUB, LANES))
            ahead = ahead + jnp.where(shifted == 0.0, 0.0, gain * shifted)
        entering = ahead
    enter = [jnp.broadcast_to(entering[:, t : t + 1], (SUB, LANES)) for t in range(steps)]
    a, b = mine[...], theirs[...]
    for t in range(steps):
        total = jnp.where(plain, a[t], b[t])
        for d in range(steps - t):
            response = jnp.where(plain, b[steps - 1 - d], a[steps - 1 - d])
            total = total + jnp.where(enter[t + d] == 0.0, 0.0, response * enter[t + d])
        for h in range(SUB // blocks):
            out[t, :, h * LANES : (h + 1) * LANES] = total[h * blocks : (h + 1) * blocks]


def join(scal, mine, theirs, far, steps, blocks):
    return pl.pallas_call(
        functools.partial(join_kernel, steps, blocks),
        out_shape=jax.ShapeDtypeStruct((steps, blocks, SUB // blocks * LANES), jnp.float32),
        in_specs=[smem()] + [vmem()] * (2 + len(far)),
        out_specs=vmem(),
        name="join",
    )(scal, mine, theirs, *far)


def exchange_rows(value, me, count, axis):
    bit = 1
    while bit < count:
        shape = value.shape
        split = value.reshape(shape[:axis] + (count // (2 * bit), 2, bit) + shape[axis + 1 :])
        other = jnp.flip(split, axis + 1).reshape(shape)
        value = jnp.where((me & bit) != 0, other, value)
        bit *= 2
    return value


def on_group(sensitivity, inverse, spread, gather_weight, retain, storage, conf_source, conf_target, conf_weight):
    steps, blocks, reaches = sensitivity.shape
    halves = reaches // LANES
    slots = conf_source.shape[2]
    count, me = lax.axis_size("reach"), lax.axis_index("reach")

    def to_rows(value):
        lead = value.shape[:-2]
        split = value.reshape(lead + (blocks, halves, LANES))
        return jnp.swapaxes(split, -3, -2).reshape(lead + (SUB, LANES))

    sent, upon = prepare(inverse, gather_weight)
    sent = sent.reshape(LANES, -1, LANES)
    x, y = swap(sent, "reach", 2), swap(sent, "reach", 4)
    near = swap(sent, "reach", 1)
    middle = LANES // 2
    diag = jnp.concatenate([swap(x[:middle], "reach", 4), swap(y[middle:], "reach", 2)], axis=0)
    pieces = [sent, near, x, swap(x, "reach", 1), y, swap(y, "reach", 1), diag, swap(diag, "reach", 1)]

    wide = jnp.concatenate([conf_source[0], conf_target[0]], axis=1).astype(jnp.float32)
    last = jnp.zeros((2 * SUB, LANES), jnp.float32).at[:count, :slots].set(conf_weight[0]).at[SUB, :blocks].set(retain)
    aux = jnp.concatenate(
        [to_rows(sensitivity).reshape(steps * SUB, LANES), to_rows(storage), to_rows(spread), upon, wide, last], axis=0
    )
    at = {name: (steps + i) * SUB for i, name in enumerate(("storage", "spread", "upon", "conf", "weight", "retain"))}
    far = jnp.stack([aux, swap(aux, "reach", 2), swap(aux, "reach", 4), swap(aux, "reach", 6)])
    aux = jnp.stack([far, swap(far, "reach", 1)], axis=1).reshape((count,) + aux.shape)

    def rows_at(name, length, first=0, width=LANES):
        return aux[:, at[name] : at[name] + length, first : first + width]

    def paired(value):
        value = value.reshape(count * slots // LANES, LANES // slots, count, slots)
        return jnp.swapaxes(value, 1, 2).reshape(-1, count, LANES)

    def coded(index):
        row = lax.rem(index, reaches) // LANES * blocks + index // reaches
        return row, lax.rem(index, LANES)

    conf = exchange_rows(rows_at("conf", count).astype(jnp.int32), me, count, 1)
    source_row, source_lane = coded(paired(conf[..., :slots]))
    target_row, target_lane = coded(conf[..., slots:])
    target = target_row * LANES + target_lane
    weight = paired(exchange_rows(rows_at("weight", count, 0, slots), me, count, 1))
    nexts, heads, most = tables(target, paired(target), slots)

    keep = rows_at("retain", 1, 0, blocks).reshape(-1)
    order = ((jnp.arange(count, dtype=jnp.int32) ^ me)[:, None] * blocks + jnp.arange(blocks, dtype=jnp.int32)).reshape(-1)
    by_row = jnp.broadcast_to(order.reshape(count, 1, blocks), (count, halves, blocks)).reshape(-1)
    to = jnp.concatenate([by_row, jnp.full((SUB,), -1, jnp.int32)])
    past = order[:, None, None] > to[None, :, None]
    chain = jnp.where(past & (order[:, None, None] < by_row[None, None, :]), keep[:, None, None], 1.0)
    links = jnp.where(by_row[None, :] > to[:, None], jnp.prod(chain, axis=0), 0.0)
    inflow = jnp.prod(jnp.where(past, keep[:, None, None], 1.0), axis=0)
    inflow = jnp.broadcast_to(inflow, (to.shape[0], LANES))

    plain = (me & 1) == 0
    scal = jnp.where(plain, jnp.array([1.0, 0.0], jnp.float32), jnp.array([0.0, 1.0], jnp.float32))
    mine, theirs = sweep(
        at, steps, scal, pieces, aux, source_lane, source_row, weight, nexts, heads, most, links, inflow
    )
    theirs = swap(theirs, "reach", 1)
    leaving = jnp.stack([mine[steps], theirs[steps]])
    leaving = jnp.where(plain, leaving, leaving[::-1])
    groups = lax.axis_size("basin")
    far = [
        lax.ppermute(leaving, "basin", [(g + d, g) for g in range(groups - d)])
        for d in reversed(range(1, groups))
    ]
    return join(scal, mine, theirs, far, steps, blocks)


def entering_2(value, axis, join, neutral):
    count, mine = (lax.axis_size(axis), lax.axis_index(axis))
    pieces = jax.tree.map(lambda part: lax.all_gather(part, axis), value)
    pieces = jax.tree.map(lambda part: part[::-1], pieces)
    mine = count - 1 - mine
    running = jax.tree.map(
        lambda part, zero: jnp.full_like(part, 0) + jnp.asarray(zero, part.dtype), value, neutral
    )

    def turn(position, running):
        longer = join(running, jax.tree.map(lambda part: part[position], pieces))
        return jax.tree.map(lambda new, old: jnp.where(position < mine, new, old), longer, running)

    return lax.fori_loop(0, count - 1, turn, running)


def from_root(value, axis, source):
    kept = jnp.where(lax.axis_index(axis) == source, value, 0).astype(value.dtype)
    return lax.psum(kept, axis)


def compose(earlier, later):
    return (later[0] * earlier[0], later[0] * earlier[1] + later[1])


def on_device(
    sensitivity,
    inverse,
    spread,
    gather_weight,
    retain,
    storage,
    conf_source,
    conf_target,
    conf_weight,
):
    blocks, reaches = spread.shape
    rows = blocks * reaches
    sources = conf_source[0]
    targets = conf_target[0].reshape(-1)
    weights = conf_weight[0]
    identity = (jnp.ones((), jnp.float32), jnp.zeros((), jnp.float32))

    def step(later, forcing_now):
        flat = later.reshape(rows)
        everyone = lax.all_gather(flat[None], "reach", axis=0, tiled=True)
        values = jnp.take_along_axis(everyone, sources, axis=1)
        fan = jnp.zeros((rows,), jnp.float32).at[targets].add((values * weights).reshape(-1))
        forcing = forcing_now + storage * later + fan.reshape(blocks, reaches)
        local = jnp.einsum("bij,bi->bj", inverse, forcing, precision=lax.Precision.HIGHEST)
        feed = jnp.sum(gather_weight * local, axis=1)
        slope = jnp.ones((), jnp.float32)
        offset = jnp.zeros((), jnp.float32)
        for block in reversed(range(blocks)):
            offset = retain[block] * offset + feed[block]
            slope = retain[block] * slope
        within = entering_2((slope, offset), "reach", compose, identity)
        inclusive = jnp.stack(compose(within, (slope, offset)))
        total = from_root(inclusive, "reach", 0)
        outer = entering_2((total[0], total[1]), "basin", compose, identity)
        prior = compose(outer, within)
        stem = prior[1]
        entering = []
        for block in reversed(range(blocks)):
            entering.append(stem)
            stem = retain[block] * stem + feed[block]
        stem_next = jnp.stack(entering[::-1])
        adjoint = local + spread * stem_next[:, None]
        return (adjoint, adjoint)

    _, adjoint = lax.scan(
        step, jnp.zeros((blocks, reaches), jnp.float32), sensitivity, reverse=True
    )
    return adjoint


def fits(args, mesh):
    steps, blocks, reaches = args[0].shape
    slots, count = args[6].shape[2], mesh.shape["reach"]
    halves = reaches // LANES
    return (
        reaches % LANES == 0
        and blocks * halves == SUB
        and count == SUB
        and count * halves * SUB == LANES
        and LANES % slots == 0
        and slots * 2 == LANES
        and steps <= LANES
    )


def solution(mesh):
    placed = (
        P(None, ("basin", "reach"), None),
        P(("basin", "reach"), None, None),
        P(("basin", "reach"), None),
        P(("basin", "reach"), None),
        P(("basin", "reach")),
        P(("basin", "reach"), None),
        P(("basin", "reach"), None, None),
        P(("basin", "reach"), None, None),
        P(("basin", "reach"), None, None),
    )
    def program(*args):
        return (on_group if fits(args, mesh) else on_device)(*args)

    return jax.shard_map(
        program,
        mesh=mesh,
        in_specs=placed,
        out_specs=P(None, ("basin", "reach"), None),
        check_vma=False,
    )
```
